256 devices in a mesh: dp: 64 (over x_lo, y, z), mp: 2 (over core), fsdp: 2 (over x_hi).
Axes of the slice: x: 4 (x_hi: 2, x_lo: 2; x = x_hi * 2 + x_lo), y: 4, z: 8, core: 2. Of those that a mesh axis runs over, the one named last changes fastest.
Arguments:
- features: bfloat16 [5, 1024, 4096], P(None, ('dp', 'fsdp')), may hold values from -24 to 24
- memory_bank: bfloat16 [4096, 32, 1024], P(('dp', 'fsdp')), may hold values from -1 to 1
- memory_fill: int32 [4096], P(('dp', 'fsdp')), may hold values from 0 to 32
- left_keys: bfloat16 [4096, 64, 1024], P(('dp', 'fsdp'), None, 'mp'), may hold values from -400 to 400
- left_values: bfloat16 [4096, 64, 1024], P(('dp', 'fsdp'), None, 'mp'), may hold values from -6 to 6
- left_length: int32 [4096], P(('dp', 'fsdp')), may hold values from 0 to 64
- w_query: bfloat16 [1024, 1024], P('fsdp', 'mp'), may hold values from -0.1875 to 0.1875
- w_key: bfloat16 [1024, 1024], P('fsdp', 'mp'), may hold values from -0.1875 to 0.1875
- w_value: bfloat16 [1024, 1024], P('fsdp', 'mp'), may hold values from -0.1875 to 0.1875
- w_out: bfloat16 [1024, 1024], P('mp', 'fsdp'), may hold values from -0.1875 to 0.1875
- w_up: bfloat16 [1024, 4096], P('fsdp', 'mp'), may hold values from -0.1875 to 0.1875
- w_down: bfloat16 [4096, 1024], P('mp', 'fsdp'), may hold values from -0.09375 to 0.09375
- out_gain: float32 [1024], replicated, may hold values from 0.1 to 1.9
Outputs:
- layer_out: bfloat16 [4096, 5, 1024], P(('dp', 'fsdp'))
- memory_next: bfloat16 [4096, 1024], P(('dp', 'fsdp'))
- center_keys: bfloat16 [4096, 4, 1024], P(('dp', 'fsdp'), None, 'mp')
- center_values: bfloat16 [4096, 4, 1024], P(('dp', 'fsdp'), None, 'mp')
The draws below stay inside these ranges and needn't reach their ends.
All inputs are finite; a program needn't handle non-finite values.
Results may differ from the reference program's by a relative error of at most 0.0095.
Values may be sent and summed in bfloat16 or wider, within the bound.
No kernel may reach another device: no remote copies, remote signals or barrier semaphores. Data moves between devices by JAX's collectives and lax.ppermute only.
A program may use at most 128 MiB of HBM per device.

```python
import jax
import jax.numpy as jnp
from jax import lax

D = 1024
H = 16
HD = 64
FF = 4096
MEM = 32
LEFT = 64
GROUP = 4
FRAMES = 5
STR_DEV = 32
STREAMS = 4096


def draw_left_keys(key, part):
    base = jnp.clip(jax.random.normal(jax.random.fold_in(key, 11), (STREAMS, LEFT, D), jnp.float32), -6.0, 6.0)
    return base.astype(jnp.bfloat16)


def set_ends(entries, key, least, top_value):
    place = [jax.random.randint(jax.random.fold_in(key, axis), (), 0, length) for axis, length in enumerate(entries.shape)]
    main_axis = entries.shape.index(max(entries.shape))
    beside = place[:main_axis] + [(place[main_axis] + 1) % entries.shape[main_axis]] + place[main_axis + 1:]
    return entries.at[tuple(place)].set(least).at[tuple(beside)].set(top_value)


def raised(values, key, source, target, parts, factor):
    def block_of(dim):
        return (jnp.arange(values.shape[dim]) // (values.shape[dim] // parts)).reshape((-1,) + (1,) * (values.ndim - 1 - dim))

    one_side = jax.random.permutation(key, parts)[block_of(target)]
    second = (block_of(target) + parts // 2) % parts
    return jnp.where((block_of(source) == one_side) | (block_of(source) == second), factor * values, values)


def levels(own_key, extent, pieces, smallest, top_value):
    level = 1.0
    for position, shards_of in pieces:
        heights = jax.random.uniform(jax.random.fold_in(jax.random.fold_in(own_key, 6), position), (shards_of,), jnp.float32, smallest / len(pieces), top_value / len(pieces))
        level = level * jnp.repeat(jnp.exp(heights), extent[position] // shards_of).reshape((-1,) + (1,) * (len(extent) - 1 - position))
    return level


def normal_values(stream_key, dims, width, most, shards=(), held_as=jnp.bfloat16):
    values = jax.random.normal(stream_key, dims, jnp.float32) * width
    if len(shards) > 0:
        values = levels(stream_key, dims, shards, -0.22, 0.18) * values
    return jnp.clip(values, min=-most, max=most).astype(held_as)


def bell_draw_with(stream_key, shape, width, limit, cuts, heavy, kind=jnp.bfloat16):
    values = width * jax.random.normal(stream_key, shape, jnp.float32)
    if cuts:
        values = values * levels(stream_key, shape, cuts, -0.22, 0.18)
    return jnp.clip(raised(values, jax.random.fold_in(stream_key, 3), *heavy), -limit, limit).astype(kind)


def setup_inputs(seed: int = 0) -> dict:
    streams_of = jax.random.split(jax.random.key(seed), 14)
    features = bell_draw_with(streams_of[0], (FRAMES, D, STREAMS), 1.0, 24.0, ((1, 128),), (1, 2, 128, 5.5))
    memory_bank = jnp.clip(jax.random.uniform(streams_of[1], (STREAMS, MEM, D), jnp.float32, -1.0, 1.0) * levels(streams_of[1], (STREAMS, MEM, D), ((0, 128),), -0.4, 0.0), -1.0, 1.0).astype(jnp.bfloat16)
    memory_fill = set_ends(jax.random.randint(streams_of[2], (STREAMS,), 0, MEM + 1), jax.random.fold_in(streams_of[2], 1), 0, MEM).astype(jnp.int32)
    left_keys = draw_left_keys(jax.random.fold_in(streams_of[13], 71), 0)
    left_values = normal_values(streams_of[4], (STREAMS, LEFT, D), 1.0, 6.0, ((0, 128), (2, 2)))
    left_length = set_ends(jax.random.randint(streams_of[5], (STREAMS,), 0, LEFT + 1), jax.random.fold_in(streams_of[5], 1), 0, LEFT).astype(jnp.int32)
    w_query = normal_values(streams_of[6], (D, D), D ** -0.5, 0.1875, ((0, 2), (1, 2)))
    w_key = normal_values(streams_of[7], (D, D), D ** -0.5, 0.1875, ((0, 2), (1, 2)))
    w_value = normal_values(streams_of[8], (D, D), D ** -0.5, 0.1875, ((0, 2), (1, 2)))
    w_out = normal_values(streams_of[9], (D, D), D ** -0.5, 0.1875, ((0, 2), (1, 2)))
    w_up = normal_values(streams_of[10], (D, FF), D ** -0.5, 0.1875, ((0, 2), (1, 2)))
    w_down = normal_values(streams_of[11], (FF, D), FF ** -0.5, 0.09375, ((0, 2), (1, 2)))
    out_gain = jnp.clip(1.0 + 0.18 * jax.random.normal(streams_of[12], (D,), jnp.float32), 0.1, 1.9)
    return {"features": features, "memory_bank": memory_bank, "memory_fill": memory_fill, "left_keys": left_keys, "left_values": left_values, "left_length": left_length, "w_query": w_query, "w_key": w_key, "w_value": w_value, "w_out": w_out, "w_up": w_up, "w_down": w_down, "out_gain": out_gain}


epsilon = 1e-05
masked_score = -1e+30

def normalize(values):
    values = values.astype(jnp.float32)
    average = lax.optimization_barrier(jnp.mean(values, axis=-1, keepdims=True))
    centred = values - average
    variance = lax.optimization_barrier(jnp.mean(centred * centred, axis=-1, keepdims=True))
    return centred * lax.rsqrt(variance + epsilon)

def visible_masks(fill, length, mem_slots, left_slots, query_count):
    mem_ok = jnp.arange(mem_slots, dtype=jnp.int32)[None, :] >= (mem_slots - fill)[:, None]
    not_summary = jnp.arange(query_count, dtype=jnp.int32) < query_count - 1
    mem_mask = mem_ok[:, None, None, :] & not_summary[None, None, :, None]
    left_ok = jnp.arange(left_slots, dtype=jnp.int32)[None, :] >= (left_slots - length)[:, None]
    left_mask = left_ok[:, None, None, :] & (not_summary[None, None, :, None] | True)
    return (mem_mask, left_mask)

def reference(features, memory_bank, memory_fill, left_keys, left_values, left_length, w_query, w_key, w_value, w_out, w_up, w_down, out_gain):
    streams = features.shape[2]
    inputs = jnp.transpose(features, (2, 0, 1))
    normed = normalize(inputs).astype(jnp.bfloat16)
    summary = lax.optimization_barrier(jnp.mean(normed[:, :GROUP, :].astype(jnp.float32), axis=1)).astype(jnp.bfloat16)
    query_rows = jnp.concatenate([normed, summary[:, None, :]], axis=1).reshape(-1, D)
    query_proj = jnp.dot(query_rows, w_query, preferred_element_type=jnp.float32).astype(jnp.bfloat16)
    group_rows = normed.reshape(-1, D)
    group_keys = jnp.dot(group_rows, w_key, preferred_element_type=jnp.float32).astype(jnp.bfloat16)
    group_values = jnp.dot(group_rows, w_value, preferred_element_type=jnp.float32).astype(jnp.bfloat16)
    blocks = streams // STR_DEV
    scale = HD ** (-0.5)

    def split(array):
        return array.reshape((blocks, STR_DEV) + array.shape[1:])

    def attend(operands):
        query_blk, ckey_blk, cval_blk, memory_blk, lkey_blk, lval_blk, fill_blk, length_blk = operands
        memory_rows = memory_blk.reshape(-1, D)
        mem_keys = jnp.dot(memory_rows, w_key, preferred_element_type=jnp.float32).astype(jnp.bfloat16)
        mem_values = jnp.dot(memory_rows, w_value, preferred_element_type=jnp.float32).astype(jnp.bfloat16)
        query_h = query_blk.reshape(STR_DEV, FRAMES + 1, H, HD).astype(jnp.float32)
        mkey_h = mem_keys.reshape(STR_DEV, MEM, H, HD).astype(jnp.float32)
        mval_h = mem_values.reshape(STR_DEV, MEM, H, HD).astype(jnp.float32)
        lkey_h = lkey_blk.reshape(STR_DEV, LEFT, H, HD).astype(jnp.float32)
        lval_h = lval_blk.reshape(STR_DEV, LEFT, H, HD).astype(jnp.float32)
        ckey_h = ckey_blk.reshape(STR_DEV, FRAMES, H, HD).astype(jnp.float32)
        cval_h = cval_blk.reshape(STR_DEV, FRAMES, H, HD).astype(jnp.float32)
        mem_mask, left_mask = visible_masks(fill_blk, length_blk, MEM, LEFT, FRAMES + 1)
        score_mem = jnp.einsum('sqhd,skhd->shqk', query_h, mkey_h) * scale
        score_left = jnp.einsum('sqhd,skhd->shqk', query_h, lkey_h) * scale
        score_group = jnp.einsum('sqhd,skhd->shqk', query_h, ckey_h) * scale
        score_mem = jnp.where(mem_mask, score_mem, masked_score)
        score_left = jnp.where(left_mask, score_left, masked_score)
        top = jnp.maximum(jnp.maximum(lax.optimization_barrier(jnp.max(score_mem, axis=-1, keepdims=True)), lax.optimization_barrier(jnp.max(score_left, axis=-1, keepdims=True))), lax.optimization_barrier(jnp.max(score_group, axis=-1, keepdims=True)))
        exp_mem = jnp.exp(score_mem - top)
        exp_left = jnp.exp(score_left - top)
        exp_group = jnp.exp(score_group - top)
        totals = lax.optimization_barrier(jnp.sum(exp_mem, axis=-1, keepdims=True)) + lax.optimization_barrier(jnp.sum(exp_left, axis=-1, keepdims=True)) + lax.optimization_barrier(jnp.sum(exp_group, axis=-1, keepdims=True))
        prob_mem = (exp_mem / totals).astype(jnp.bfloat16).astype(jnp.float32)
        prob_left = (exp_left / totals).astype(jnp.bfloat16).astype(jnp.float32)
        prob_group = (exp_group / totals).astype(jnp.bfloat16).astype(jnp.float32)
        attended = jnp.einsum('shqk,skhd->sqhd', prob_mem, mval_h) + jnp.einsum('shqk,skhd->sqhd', prob_left, lval_h) + jnp.einsum('shqk,skhd->sqhd', prob_group, cval_h)
        return attended.astype(jnp.bfloat16).reshape(STR_DEV, FRAMES + 1, D)
    attended = lax.map(attend, (split(query_proj.reshape(streams, (FRAMES + 1) * D)), split(group_keys.reshape(streams, FRAMES * D)), split(group_values.reshape(streams, FRAMES * D)), split(memory_bank), split(left_keys), split(left_values), split(memory_fill), split(left_length)))
    attended = attended.reshape(-1, D)
    attn_out = jnp.dot(attended, w_out, preferred_element_type=jnp.float32).reshape(streams, FRAMES + 1, D)
    memory_next = jnp.tanh(attn_out[:, FRAMES, :]).astype(jnp.bfloat16)
    hidden_state = inputs.astype(jnp.float32) + attn_out[:, :FRAMES, :]
    h_norm = normalize(hidden_state).astype(jnp.bfloat16).reshape(-1, D)
    up_proj = jax.nn.gelu(jnp.dot(h_norm, w_up, preferred_element_type=jnp.float32), approximate=True).astype(jnp.bfloat16)
    down_proj = jnp.dot(up_proj, w_down, preferred_element_type=jnp.float32)
    layer_out = (normalize(hidden_state.reshape(-1, D) + down_proj) * out_gain.astype(jnp.float32)).astype(jnp.bfloat16).reshape(streams, FRAMES, D)
    center_keys = group_keys.reshape(streams, FRAMES, D)[:, :GROUP, :]
    center_values = group_values.reshape(streams, FRAMES, D)[:, :GROUP, :]
    return (layer_out, memory_next, center_keys, center_values)
```

```python
import functools

import jax
import jax.numpy as jnp
from jax import lax
from jax.experimental import pallas as pl
from jax.experimental.pallas import tpu as pltpu
from jax.sharding import PartitionSpec as P

HD = 64
GROUP = 4
SLOTS = 128
epsilon = 1e-05
masked_score = -1e30
BF = jnp.bfloat16
F32 = jnp.float32
GRID = ("dp", "fsdp")
NX, NY, NZ = 2, 4, 8
PARTS = 4


def routes(move):
    def index(x, y, z, half):
        return ((x * NY + y) * NZ + z) * 2 + half

    return [
        (index(x, y, z, h), index(*move(x, y, z, h)))
        for x in range(NX)
        for y in range(NY)
        for z in range(NZ)
        for h in range(2)
    ]


ACROSS = routes(lambda x, y, z, h: (1 - x, y, z, 1 - h))
TO_Y_BELOW = routes(lambda x, y, z, h: (x, (y - 1) % NY, z, h))
TO_Y_ABOVE = routes(lambda x, y, z, h: (x, (y + 1) % NY, z, h))
TO_Z_BELOW = routes(lambda x, y, z, h: (x, y, (z - 1) % NZ, h))
TO_Z_ABOVE = routes(lambda x, y, z, h: (x, y, (z + 1) % NZ, h))


def colour():
    dp = lax.axis_index("dp")
    return lax.rem(lax.rem(dp // NZ, NY) + 2 * lax.rem(dp, NZ), PARTS)


def spread(piece, along_z):
    return (
        piece,
        lax.ppermute(piece, GRID, TO_Y_BELOW),
        lax.ppermute(piece, GRID, along_z),
        lax.ppermute(piece, GRID, TO_Y_ABOVE),
    )


def normalize(values):
    average = jnp.mean(values, axis=-1, keepdims=True)
    centred = values - average
    variance = jnp.mean(centred * centred, axis=-1, keepdims=True)
    return centred * lax.rsqrt(variance + epsilon)


def matmul(left, right):
    return jnp.dot(left, right, preferred_element_type=F32)


def pack_kernel(feat_ref, out_ref):
    frames, width_dev, all_streams = feat_ref.shape
    lanes = lax.broadcasted_iota(jnp.int32, (width_dev, 128), 1)
    for tile in range(all_streams // 128):
        block = [feat_ref[f, :, tile * 128 : tile * 128 + 128].astype(F32) for f in range(frames)]
        for k in range(4):
            rolled = [
                block[f] if (32 * (f - k)) % 128 == 0 else pltpu.roll(block[f], (32 * (f - k)) % 128, 1)
                for f in range(frames)
            ]
            first = jnp.where(
                lanes < 64,
                jnp.where(lanes < 32, rolled[0], rolled[1]),
                jnp.where(lanes < 96, rolled[2], rolled[3]),
            )
            out_ref[tile * 4 + k, :, 0:128] = first.astype(BF)
            out_ref[tile * 4 + k, :, 128:256] = jnp.where(lanes < 32, rolled[4], 0.0).astype(BF)


def pack(features):
    frames, width_dev, all_streams = features.shape
    return pl.pallas_call(
        pack_kernel,
        out_shape=jax.ShapeDtypeStruct((all_streams // 32, width_dev, 256), BF),
        in_specs=[pl.BlockSpec(memory_space=pltpu.VMEM)],
        out_specs=pl.BlockSpec(memory_space=pltpu.VMEM),
        name="pack",
    )(features)


def scatter(values, scratch, count, streams, stride):
    for f in range(count):
        for t in range(scratch.shape[0]):
            scratch[t, pl.ds(f, streams, stride=stride), :] = values[
                f * streams : (f + 1) * streams, t * 128 : t * 128 + 128
            ]


def attend_kernel(
    fill_ref, length_ref, arrived_ref, memory_ref, lkeys_ref, lvalues_ref,
    wq_ref, wk_ref, wv_ref, wo_ref, p0_ref, p1_ref, p2_ref, p3_ref,
    inputs_ref, part_ref, ckeys_ref, cvalues_ref,
    rows, keys, values, memory, weights, w_out, query_s, key_s, value_s, attended, sem,
):
    streams, mem_slots, width = memory_ref.shape
    left_slots, head_cols = lkeys_ref.shape[1:]
    half = lax.axis_index("fsdp")
    own = pl.multiple_of(half * 512, 512)
    other = pl.multiple_of((1 - half) * 512, 512)
    base = colour()
    copies = [
        pltpu.make_async_copy(wq_ref, weights.at[pl.ds(own, 512), 0:512], sem.at[0]),
        pltpu.make_async_copy(wk_ref, weights.at[pl.ds(own, 512), 512:1024], sem.at[1]),
        pltpu.make_async_copy(wv_ref, weights.at[pl.ds(own, 512), 1024:1536], sem.at[2]),
    ]
    late = [pltpu.make_async_copy(wo_ref, w_out.at[:, pl.ds(own, 512)], sem.at[3])]
    for n, piece in enumerate((p0_ref, p1_ref, p2_ref, p3_ref)):
        which = lax.rem(base + n, PARTS)
        row = pl.multiple_of(other + which * 128, 128)
        copies.append(
            pltpu.make_async_copy(piece.at[:, 0:1536], weights.at[pl.ds(row, 128), :], sem.at[4 + n])
        )
        row = pl.multiple_of(which * 128, 128)
        late.append(
            pltpu.make_async_copy(
                piece.at[:, 1536:2048], w_out.at[pl.ds(row, 128), pl.ds(other, 512)], sem.at[8 + n]
            )
        )
    fetch_memory = pltpu.make_async_copy(memory_ref, memory, sem.at[12])
    left = [
        pltpu.make_async_copy(lkeys_ref, keys.at[:, 0:left_slots, :], sem.at[13]),
        pltpu.make_async_copy(lvalues_ref, values.at[:, 0:left_slots, :], sem.at[14]),
    ]
    for copy in copies:
        copy.start()
    fetch_memory.start()
    for copy in left + late:
        copy.start()

    arrived = arrived_ref[...].astype(F32).reshape(width, 256)
    inputs = jnp.concatenate(
        [jnp.transpose(arrived[:, 0:128]), jnp.transpose(arrived[:, 128:256])[0:streams, :]], axis=0
    )
    inputs_ref[...] = inputs.astype(BF)
    frame_rows = inputs.shape[0]
    normed = normalize(inputs).astype(BF)
    rows[0:frame_rows, :] = normed
    total = normed[0:streams, :].astype(F32)
    for f in range(1, GROUP):
        total = total + normed[f * streams : (f + 1) * streams, :].astype(F32)
    rows[frame_rows : frame_rows + streams, :] = (total * (1.0 / GROUP)).astype(BF)

    key_s[...] = jnp.zeros_like(key_s)
    value_s[...] = jnp.zeros_like(value_s)
    query_s[...] = jnp.zeros_like(query_s)
    for copy in copies:
        copy.wait()
    count = frame_rows // streams
    projected = matmul(rows[...], weights[:, 0:512])
    scatter(projected, query_s, count + 1, streams, 8)
    projected = matmul(rows[...], weights[:, 512:1024])
    scatter(projected, key_s, count, streams, 16)
    projected = matmul(rows[...], weights[:, 1024:1536])
    scatter(projected, value_s, count, streams, 16)
    top_slot = left_slots + mem_slots
    for scratch, slots, out in ((key_s, keys, ckeys_ref), (value_s, values, cvalues_ref)):
        for tile in range(head_cols // 128):
            cols = slice(tile * 128, tile * 128 + 128)
            grouped = scratch[tile].reshape(streams, 16, 128)
            out[:, :, cols] = grouped[:, 0:GROUP, :].astype(BF)
            slots[:, top_slot : top_slot + 16, cols] = grouped.astype(BF)
        slots[:, top_slot + 16 : SLOTS, :] = jnp.zeros((streams, SLOTS - top_slot - 16, head_cols), BF)

    fetch_memory.wait()
    for block in range(4):
        lines = memory[block * 8 : block * 8 + 8].reshape(8 * mem_slots, width)
        at = slice(block * 8, block * 8 + 8)
        projected = matmul(lines, weights[:, 512:1024]).astype(BF)
        keys[at, left_slots:top_slot, :] = projected.reshape(8, mem_slots, head_cols)
        projected = matmul(lines, weights[:, 1024:1536]).astype(BF)
        values[at, left_slots:top_slot, :] = projected.reshape(8, mem_slots, head_cols)
    for copy in left:
        copy.wait()

    heads = head_cols // HD
    line = lax.broadcasted_iota(jnp.int32, (heads * 8, head_cols), 0)
    column = lax.broadcasted_iota(jnp.int32, (heads * 8, head_cols), 1)
    same_head = (line // 8) == (column // HD)
    slot = lax.broadcasted_iota(jnp.int32, (heads * 8, SLOTS), 1)
    asks = lax.rem(lax.broadcasted_iota(jnp.int32, (heads * 8, SLOTS), 0), 8)
    in_left = slot < left_slots
    in_mem = (slot >= left_slots) & (slot < top_slot) & (asks != count)
    in_group = (slot >= top_slot) & (slot < top_slot + count)

    def one_stream(s, carry):
        at = pl.multiple_of(s * 8, 8)
        query = jnp.concatenate([query_s[t, pl.ds(at, 8), :] for t in range(head_cols // 128)], axis=1)
        spread_q = jnp.where(same_head, jnp.concatenate([query] * heads, axis=0), 0.0).astype(BF)
        scores = lax.dot_general(
            spread_q, keys[s], (((1,), (1,)), ((), ())), preferred_element_type=F32
        ) * (HD ** -0.5)
        seen = (
            (in_left & (slot >= left_slots - length_ref[s]))
            | (in_mem & (slot >= top_slot - fill_ref[s]))
            | in_group
        )
        scores = jnp.where(seen, scores, masked_score)
        top = jnp.max(scores, axis=-1, keepdims=True)
        powers = jnp.exp(scores - top)
        probs = (powers / jnp.sum(powers, axis=-1, keepdims=True)).astype(BF)
        mixed = jnp.where(same_head, matmul(probs, values[s]), 0.0)
        gathered = mixed[0:8, :]
        for h in range(1, heads):
            gathered = gathered + mixed[h * 8 : h * 8 + 8, :]
        for t in range(head_cols // 128):
            query_s[t, pl.ds(at, 8), :] = gathered[:, t * 128 : t * 128 + 128]
        return carry

    lax.fori_loop(0, streams, one_stream, 0, unroll=4)

    for copy in late:
        copy.wait()
    for f in range(count + 1):
        for t in range(head_cols // 128):
            attended[f * streams : (f + 1) * streams, t * 128 : t * 128 + 128] = query_s[
                t, pl.ds(f, streams, stride=8), :
            ].astype(BF)
    part_ref[...] = matmul(attended[...], w_out[...]).astype(BF)


def attend(fill, length, arrived, memory, lkeys, lvalues, wq, wk, wv, wo, pieces):
    streams, mem_slots, width = memory.shape
    head_cols = lkeys.shape[2]
    smem = pl.BlockSpec(memory_space=pltpu.SMEM)
    vmem = pl.BlockSpec(memory_space=pltpu.VMEM)
    hbm = pl.BlockSpec(memory_space=pl.ANY)
    frames = 5
    return pl.pallas_call(
        attend_kernel,
        out_shape=(
            jax.ShapeDtypeStruct((frames * streams, width), BF),
            jax.ShapeDtypeStruct(((frames + 1) * streams, width), BF),
            jax.ShapeDtypeStruct((streams, GROUP, head_cols), BF),
            jax.ShapeDtypeStruct((streams, GROUP, head_cols), BF),
        ),
        in_specs=[smem, smem, vmem] + [hbm] * 11,
        out_specs=(vmem,) * 4,
        scratch_shapes=[
            pltpu.VMEM(((frames + 1) * streams, width), BF),
            pltpu.VMEM((streams, SLOTS, head_cols), BF),
            pltpu.VMEM((streams, SLOTS, head_cols), BF),
            pltpu.VMEM((streams, mem_slots, width), BF),
            pltpu.VMEM((width, 3 * head_cols), BF),
            pltpu.VMEM((head_cols, width), BF),
            pltpu.VMEM((head_cols // 128, streams * 8, 128), F32),
            pltpu.VMEM((head_cols // 128, streams * 16, 128), F32),
            pltpu.VMEM((head_cols // 128, streams * 16, 128), F32),
            pltpu.VMEM(((frames + 1) * streams, head_cols), BF),
            pltpu.SemaphoreType.DMA((15,)),
        ],
        compiler_params=pltpu.CompilerParams(vmem_limit_bytes=48 * 2**20),
        cost_estimate=pl.CostEstimate(flops=6 * 10**9, bytes_accessed=12 * 10**6, transcendentals=0),
        name="attend",
    )(fill, length, arrived, memory, lkeys, lvalues, wq, wk, wv, wo, *pieces)


def feed_kernel(
    part_ref, mate_ref, inputs_ref, wu_ref, u0_ref, u1_ref, u2_ref, u3_ref,
    wd_ref, d0_ref, d1_ref, d2_ref, d3_ref,
    state_ref, next_ref, down_ref, w_up, w_down, sem,
):
    half = lax.axis_index("fsdp")
    own = pl.multiple_of(half * 512, 512)
    other = pl.multiple_of((1 - half) * 512, 512)
    base = colour()
    ups = [pltpu.make_async_copy(wu_ref, w_up.at[pl.ds(own, 512), :], sem.at[0])]
    downs = [pltpu.make_async_copy(wd_ref, w_down.at[:, pl.ds(own, 512)], sem.at[1])]
    for n, piece in enumerate((u0_ref, u1_ref, u2_ref, u3_ref)):
        row = pl.multiple_of(other + lax.rem(base + n, PARTS) * 128, 128)
        ups.append(pltpu.make_async_copy(piece, w_up.at[pl.ds(row, 128), :], sem.at[2 + n]))
    for n, piece in enumerate((d0_ref, d1_ref, d2_ref, d3_ref)):
        row = pl.multiple_of(lax.rem(base + n, PARTS) * 512, 512)
        downs.append(
            pltpu.make_async_copy(piece, w_down.at[pl.ds(row, 512), pl.ds(other, 512)], sem.at[6 + n])
        )
    for copy in ups + downs:
        copy.start()
    frame_rows = inputs_ref.shape[0]
    attn_out = part_ref[...].astype(F32) + mate_ref[...].astype(F32)
    next_ref[...] = jnp.tanh(attn_out[frame_rows:, :]).astype(BF)
    state = inputs_ref[...].astype(F32) + attn_out[0:frame_rows, :]
    state_ref[...] = state
    h_norm = normalize(state).astype(BF)
    for copy in ups:
        copy.wait()
    hidden = jax.nn.gelu(matmul(h_norm, w_up[...]), approximate=True).astype(BF)
    for copy in downs:
        copy.wait()
    down_ref[...] = matmul(hidden, w_down[...]).astype(BF)


def feed(part, mate, inputs, w_up, up_pieces, w_down, down_pieces):
    frame_rows, width = inputs.shape
    vmem = pl.BlockSpec(memory_space=pltpu.VMEM)
    hbm = pl.BlockSpec(memory_space=pl.ANY)
    units = w_up.shape[1]
    return pl.pallas_call(
        feed_kernel,
        out_shape=(
            jax.ShapeDtypeStruct((frame_rows, width), F32),
            jax.ShapeDtypeStruct((part.shape[0] - frame_rows, width), BF),
            jax.ShapeDtypeStruct((frame_rows, width), BF),
        ),
        in_specs=[vmem] * 3 + [hbm] * 10,
        out_specs=(vmem,) * 3,
        scratch_shapes=[
            pltpu.VMEM((width, units), BF),
            pltpu.VMEM((units, width), BF),
            pltpu.SemaphoreType.DMA((10,)),
        ],
        compiler_params=pltpu.CompilerParams(vmem_limit_bytes=40 * 2**20),
        cost_estimate=pl.CostEstimate(flops=3 * 10**9, bytes_accessed=10 * 10**6, transcendentals=0),
        name="feed",
    )(part, mate, inputs, w_up, *up_pieces, w_down, *down_pieces)


def finish_kernel(state_ref, down_ref, mate_ref, gain_ref, out_ref):
    down = down_ref[...].astype(F32) + mate_ref[...].astype(F32)
    result = normalize(state_ref[...] + down) * gain_ref[...]
    out_ref[...] = result.astype(BF).reshape(out_ref.shape)


def finish(state, down, mate, gain, streams):
    vmem = pl.BlockSpec(memory_space=pltpu.VMEM)
    return pl.pallas_call(
        finish_kernel,
        out_shape=jax.ShapeDtypeStruct((state.shape[0] // streams, streams, state.shape[1]), BF),
        in_specs=[vmem] * 4,
        out_specs=vmem,
        name="finish",
    )(state, down, mate, gain[None, :])


def shards(
    features, memory_bank, memory_fill, left_keys, left_values, left_length,
    w_query, w_key, w_value, w_out, w_up, w_down, out_gain,
):
    streams = memory_bank.shape[0]
    swap = [(0, 1), (1, 0)]
    at = colour()

    def mine(w, rows):
        return lax.dynamic_slice_in_dim(w, at * rows, rows, axis=0)

    first = jnp.concatenate([mine(w, 128) for w in (w_query, w_key, w_value, w_out)], axis=1)
    first = lax.ppermute(first, GRID, ACROSS)
    up = lax.ppermute(mine(w_up, 128), GRID, ACROSS)
    down = lax.ppermute(mine(w_down, 512), GRID, ACROSS)

    arrived = lax.all_to_all(pack(features), GRID, split_axis=0, concat_axis=0, tiled=True)
    pieces = spread(first, TO_Z_BELOW)
    up_pieces = spread(up, TO_Z_ABOVE)
    down_pieces = spread(down, TO_Z_BELOW)
    inputs, part, center_keys, center_values = attend(
        memory_fill, left_length, arrived, memory_bank, left_keys, left_values,
        w_query, w_key, w_value, w_out, pieces,
    )
    mate = lax.ppermute(part, "mp", swap)
    state, memory_next, down_part = feed(part, mate, inputs, w_up, up_pieces, w_down, down_pieces)
    down_mate = lax.ppermute(down_part, "mp", swap)
    out = finish(state, down_part, down_mate, out_gain, streams)
    return (jnp.transpose(out, (1, 0, 2)), memory_next, center_keys, center_values)


def solution(mesh):
    in_specs = (
        P(None, ("dp", "fsdp"), None),
        P(("dp", "fsdp"), None, None),
        P(("dp", "fsdp")),
        P(("dp", "fsdp"), None, "mp"),
        P(("dp", "fsdp"), None, "mp"),
        P(("dp", "fsdp")),
        P("fsdp", "mp"),
        P("fsdp", "mp"),
        P("fsdp", "mp"),
        P("mp", "fsdp"),
        P("fsdp", "mp"),
        P("mp", "fsdp"),
        P(),
    )
    out_specs = (
        P(("dp", "fsdp"), None, None),
        P(("dp", "fsdp"), None),
        P(("dp", "fsdp"), None, "mp"),
        P(("dp", "fsdp"), None, "mp"),
    )
    return jax.shard_map(shards, mesh=mesh, in_specs=in_specs, out_specs=out_specs, check_vma=False)
```

```python
import jax
import jax.numpy as jnp
from jax import lax
from jax.experimental import pallas as pl
from jax.experimental.pallas import tpu as pltpu
from jax.sharding import PartitionSpec as P

HD = 64
GROUP = 4
FRAMES = 5
TOGETHER = 16
SLOTS = 128
epsilon = 1e-05
masked_score = -1e30
BF = jnp.bfloat16
F32 = jnp.float32
GRID = ("dp", "fsdp")
NX, NY, NZ = 2, 4, 8
PARTS = 4
WHOLE = 67_000_000
ROOM = 16_000_000


def routes(move):
    def index(x, y, z, half):
        return ((x * NY + y) * NZ + z) * 2 + half

    return [
        (index(x, y, z, h), index(*move(x, y, z, h)))
        for x in range(NX)
        for y in range(NY)
        for z in range(NZ)
        for h in range(2)
    ]


ACROSS = routes(lambda x, y, z, h: (1 - x, y, z, 1 - h))
TO_Y_BELOW = routes(lambda x, y, z, h: (x, (y - 1) % NY, z, h))
TO_Y_ABOVE = routes(lambda x, y, z, h: (x, (y + 1) % NY, z, h))
TO_Z_BELOW = routes(lambda x, y, z, h: (x, y, (z - 1) % NZ, h))
TO_Z_ABOVE = routes(lambda x, y, z, h: (x, y, (z + 1) % NZ, h))


def colour():
    dp = lax.axis_index("dp")
    return lax.rem(lax.rem(dp // NZ, NY) + 2 * lax.rem(dp, NZ), PARTS)


def hop(piece, route):
    return lax.ppermute(piece, GRID, route)


def spread(piece, along_z):
    return (piece, hop(piece, TO_Y_BELOW), hop(piece, along_z), hop(piece, TO_Y_ABOVE))


def normalize(values):
    average = jnp.mean(values, axis=-1, keepdims=True)
    centred = values - average
    variance = jnp.mean(centred * centred, axis=-1, keepdims=True)
    return centred * lax.rsqrt(variance + epsilon)


def matmul(left, right):
    return jnp.dot(left, right, preferred_element_type=F32)


def prepare_kernel(
    feat_ref, wq_ref, wk_ref, wv_ref, wo_ref, wu_ref, wd_ref,
    out_ref, first, up, down, sem,
):
    row = pl.multiple_of(colour() * 128, 128)
    loads = [
        pltpu.make_async_copy(
            w.at[pl.ds(row, 128), :], first.at[:, n * 512 : n * 512 + 512], sem.at[n]
        )
        for n, w in enumerate((wq_ref, wk_ref, wv_ref, wo_ref))
    ]
    row = pl.multiple_of(colour() * 128, 128)
    loads.append(pltpu.make_async_copy(wu_ref.at[pl.ds(row, 128), :], up, sem.at[4]))
    row = pl.multiple_of(colour() * 512, 512)
    loads.append(pltpu.make_async_copy(wd_ref.at[pl.ds(row, 512), :], down, sem.at[5]))
    for copy in loads:
        copy.start()

    frames, width_dev, all_streams = feat_ref.shape
    tiles = all_streams // 128
    core = lax.axis_index("mp")
    shape = (frames * 128, 4 * 128)
    source = lax.broadcasted_iota(jnp.int32, shape, 0)
    target = lax.broadcasted_iota(jnp.int32, shape, 1)
    frame, lane = source // 128, lax.rem(source, 128)
    which, slot = target // 128, lax.rem(target, 128)
    picks = (
        (slot // 16 == frame) & (lane // 16 == 2 * which + core) & (lax.rem(lane, 16) == lax.rem(slot, 16))
    )
    blocks = [
        jnp.concatenate(
            [feat_ref[f, :, t * 128 : t * 128 + 128].astype(F32) for f in range(frames)], axis=1
        )
        for t in range(tiles)
    ]
    packed = matmul(jnp.concatenate(blocks, axis=0).astype(BF), jnp.where(picks, 1.0, 0.0).astype(BF))
    for t in range(tiles):
        for k in range(4):
            block = packed[t * width_dev : (t + 1) * width_dev, k * 128 : k * 128 + 128]
            out_ref[t * 4 + k] = block.astype(BF)
    for copy in loads:
        copy.wait()


def prepare(features, wq, wk, wv, wo, wu, wd):
    hbm = pl.BlockSpec(memory_space=pltpu.HBM)
    vmem = pl.BlockSpec(memory_space=pltpu.VMEM)
    shapes = ((128, 2048), (128, wu.shape[1]), (512, wd.shape[1]))
    parts = (features.shape[2] // 32, features.shape[1], 128)
    return pl.pallas_call(
        prepare_kernel,
        out_shape=tuple(jax.ShapeDtypeStruct(shape, BF) for shape in (parts,) + shapes),
        in_specs=[vmem] + [hbm] * 6,
        out_specs=(vmem,) * 4,
        scratch_shapes=[pltpu.SemaphoreType.DMA((6,))],
        compiler_params=pltpu.CompilerParams(vmem_limit_bytes=WHOLE - 3 * 10**6),
        name="prepare",
    )(features, wq, wk, wv, wo, wu, wd)


def stage_feed_kernel(wu_ref, wd_ref, w_up, w_down, sem):
    own = pl.multiple_of(lax.axis_index("fsdp") * 512, 512)
    copies = [
        pltpu.make_async_copy(wu_ref, w_up.at[pl.ds(own, 512), :], sem.at[0]),
        pltpu.make_async_copy(wd_ref, w_down.at[:, pl.ds(own, 512)], sem.at[1]),
    ]
    for copy in copies:
        copy.start()
    for copy in copies:
        copy.wait()


def stage_feed(wu, wd):
    hbm = pl.BlockSpec(memory_space=pltpu.HBM)
    width, units = 2 * wu.shape[0], wu.shape[1]
    return pl.pallas_call(
        stage_feed_kernel,
        out_shape=(
            jax.ShapeDtypeStruct((width, units), BF),
            jax.ShapeDtypeStruct((units, width), BF),
        ),
        in_specs=[hbm] * 2,
        out_specs=(pl.BlockSpec(memory_space=pltpu.VMEM),) * 2,
        scratch_shapes=[pltpu.SemaphoreType.DMA((2,))],
        compiler_params=pltpu.CompilerParams(vmem_limit_bytes=ROOM),
        name="stage_feed",
    )(wu, wd)


def scatter(values, scratch, count, streams, stride):
    for f in range(count):
        for t in range(scratch.shape[0]):
            scratch[t, pl.ds(f, streams, stride=stride), :] = values[
                f * streams : (f + 1) * streams, t * 128 : t * 128 + 128
            ]


def attend_kernel(
    fill_ref, length_ref, arrived_ref, mate_ref, memory_ref, lkeys_ref, lvalues_ref,
    wq_ref, wk_ref, wv_ref, wo_ref, p0_ref, p1_ref, p2_ref, p3_ref,
    inputs_ref, part_ref, ckeys_ref, cvalues_ref,
    rows, keys, values, memory, weights, w_out, query_s, key_s, value_s, mixed_s, attended, sem,
):
    streams, mem_slots, width = memory_ref.shape
    left_slots, head_cols = lkeys_ref.shape[1:]
    half = lax.axis_index("fsdp")
    own = pl.multiple_of(half * 512, 512)
    other = pl.multiple_of((1 - half) * 512, 512)
    base = colour()
    copies = [
        pltpu.make_async_copy(wq_ref, weights.at[pl.ds(own, 512), 0:512], sem.at[0]),
        pltpu.make_async_copy(wk_ref, weights.at[pl.ds(own, 512), 512:1024], sem.at[1]),
        pltpu.make_async_copy(wv_ref, weights.at[pl.ds(own, 512), 1024:1536], sem.at[2]),
    ]
    late = [pltpu.make_async_copy(wo_ref, w_out.at[:, pl.ds(own, 512)], sem.at[3])]
    for n, piece in enumerate((p0_ref, p1_ref, p2_ref, p3_ref)):
        which = lax.rem(base + n, PARTS)
        row = pl.multiple_of(other + which * 128, 128)
        copies.append(
            pltpu.make_async_copy(piece.at[:, 0:1536], weights.at[pl.ds(row, 128), :], sem.at[4 + n])
        )
        row = pl.multiple_of(which * 128, 128)
        late.append(
            pltpu.make_async_copy(
                piece.at[:, 1536:2048], w_out.at[pl.ds(row, 128), pl.ds(other, 512)], sem.at[8 + n]
            )
        )
    fetch_memory = pltpu.make_async_copy(memory_ref, memory, sem.at[12])
    left = [
        pltpu.make_async_copy(lkeys_ref, keys.at[:, 0:left_slots, :], sem.at[13]),
        pltpu.make_async_copy(lvalues_ref, values.at[:, 0:left_slots, :], sem.at[14]),
    ]
    for copy in copies:
        copy.start()
    fetch_memory.start()
    for copy in left + late:
        copy.start()

    here = arrived_ref[...].astype(F32).reshape(width, 128)
    there = mate_ref[...].astype(F32).reshape(width, 128)
    second = lax.axis_index("mp") == 1
    low = jnp.transpose(jnp.where(second, there, here))
    high = jnp.transpose(jnp.where(second, here, there))
    inputs = jnp.concatenate(
        [part[16 * f : 16 * f + 16, :] for f in range(FRAMES) for part in (low, high)], axis=0
    )
    inputs_ref[...] = inputs.astype(BF)
    frame_rows = inputs.shape[0]
    normed = normalize(inputs).astype(BF)
    rows[0:frame_rows, :] = normed
    total = normed[0:streams, :].astype(F32)
    for f in range(1, GROUP):
        total = total + normed[f * streams : (f + 1) * streams, :].astype(F32)
    rows[frame_rows : frame_rows + streams, :] = (total * (1.0 / GROUP)).astype(BF)

    key_s[...] = jnp.zeros_like(key_s)
    value_s[...] = jnp.zeros_like(value_s)
    query_s[...] = jnp.zeros_like(query_s)
    for copy in copies:
        copy.wait()
    count = frame_rows // streams
    projected = matmul(rows[...], weights[:, 0:512])
    scatter(projected, query_s, count + 1, streams, 8)
    projected = matmul(rows[...], weights[:, 512:1024])
    scatter(projected, key_s, count, streams, 16)
    projected = matmul(rows[...], weights[:, 1024:1536])
    scatter(projected, value_s, count, streams, 16)
    top_slot = left_slots + mem_slots
    for scratch, slots, out in ((key_s, keys, ckeys_ref), (value_s, values, cvalues_ref)):
        for tile in range(head_cols // 128):
            cols = slice(tile * 128, tile * 128 + 128)
            grouped = scratch[tile].reshape(streams, 16, 128)
            out[:, :, cols] = grouped[:, 0:GROUP, :].astype(BF)
            slots[:, top_slot : top_slot + 16, cols] = grouped.astype(BF)
        slots[:, top_slot + 16 : SLOTS, :] = jnp.zeros((streams, SLOTS - top_slot - 16, head_cols), BF)

    fetch_memory.wait()
    for block in range(4):
        lines = memory[block * 8 : block * 8 + 8].reshape(8 * mem_slots, width)
        at = slice(block * 8, block * 8 + 8)
        projected = matmul(lines, weights[:, 512:1024]).astype(BF)
        keys[at, left_slots:top_slot, :] = projected.reshape(8, mem_slots, head_cols)
        projected = matmul(lines, weights[:, 1024:1536]).astype(BF)
        values[at, left_slots:top_slot, :] = projected.reshape(8, mem_slots, head_cols)
    for copy in left:
        copy.wait()

    heads = head_cols // HD
    line = lax.broadcasted_iota(jnp.int32, (heads * 8, head_cols), 0)
    column = lax.broadcasted_iota(jnp.int32, (heads * 8, head_cols), 1)
    same_head = (line // 8) == (column // HD)
    slot = lax.broadcasted_iota(jnp.int32, (heads * 8, SLOTS), 1)
    asks = lax.rem(lax.broadcasted_iota(jnp.int32, (heads * 8, SLOTS), 0), 8)
    in_left = slot < left_slots
    in_mem = (slot >= left_slots) & (slot < top_slot) & (asks != count)
    in_group = (slot >= top_slot) & (slot < top_slot + count)

    tiles = head_cols // 128
    lines = heads * 8

    def some_streams(n, carry):
        first = n * TOGETHER
        at = pl.multiple_of(first * 8, 8 * TOGETHER)
        query = jnp.concatenate([query_s[t, pl.ds(at, 8 * TOGETHER), :] for t in range(tiles)], axis=1)
        scores = []
        for g in range(TOGETHER):
            copies = jnp.concatenate([query[g * 8 : g * 8 + 8, :]] * heads, axis=0)
            score = lax.dot_general(
                jnp.where(same_head, copies, 0.0).astype(BF),
                keys[first + g],
                (((1,), (1,)), ((), ())),
                preferred_element_type=F32,
            ) * (HD ** -0.5)
            seen = (
                (in_left & (slot >= left_slots - length_ref[first + g]))
                | (in_mem & (slot >= top_slot - fill_ref[first + g]))
                | in_group
            )
            scores.append(jnp.where(seen, score, masked_score))
        scores = jnp.concatenate(scores, axis=0)
        powers = jnp.exp(scores - jnp.max(scores, axis=-1, keepdims=True))
        probs = (powers / jnp.sum(powers, axis=-1, keepdims=True)).astype(BF)
        for g in range(TOGETHER):
            mixed = matmul(probs[g * lines : (g + 1) * lines, :], values[first + g])
            mixed = jnp.where(same_head, mixed, 0.0)
            gathered = mixed[0:8, :]
            for h in range(1, heads):
                gathered = gathered + mixed[h * 8 : h * 8 + 8, :]
            for t in range(tiles):
                mixed_s[t, pl.ds(at + g * 8, 8), :] = gathered[:, t * 128 : t * 128 + 128]
        return carry

    lax.fori_loop(0, streams // TOGETHER, some_streams, 0)

    for copy in late:
        copy.wait()
    for f in range(count + 1):
        for t in range(head_cols // 128):
            attended[f * streams : (f + 1) * streams, t * 128 : t * 128 + 128] = mixed_s[
                t, pl.ds(f, streams, stride=8), :
            ].astype(BF)
    part_ref[...] = matmul(attended[...], w_out[...]).astype(BF)


def attend(fill, length, arrived, mate, memory, lkeys, lvalues, wq, wk, wv, wo, pieces):
    streams, mem_slots, width = memory.shape
    head_cols = lkeys.shape[2]
    smem = pl.BlockSpec(memory_space=pltpu.SMEM)
    vmem = pl.BlockSpec(memory_space=pltpu.VMEM)
    hbm = pl.BlockSpec(memory_space=pltpu.HBM)
    frames = FRAMES
    return pl.pallas_call(
        attend_kernel,
        out_shape=(
            jax.ShapeDtypeStruct((frames * streams, width), BF),
            jax.ShapeDtypeStruct(((frames + 1) * streams, width), BF),
            jax.ShapeDtypeStruct((streams, GROUP, head_cols), BF),
            jax.ShapeDtypeStruct((streams, GROUP, head_cols), BF),
        ),
        in_specs=[smem, smem, vmem, vmem] + [hbm] * 11,
        out_specs=(vmem,) * 4,
        scratch_shapes=[
            pltpu.VMEM(((frames + 1) * streams, width), BF),
            pltpu.VMEM((streams, SLOTS, head_cols), BF),
            pltpu.VMEM((streams, SLOTS, head_cols), BF),
            pltpu.VMEM((streams, mem_slots, width), BF),
            pltpu.VMEM((width, 3 * head_cols), BF),
            pltpu.VMEM((head_cols, width), BF),
            pltpu.VMEM((head_cols // 128, streams * 8, 128), F32),
            pltpu.VMEM((head_cols // 128, streams * 16, 128), F32),
            pltpu.VMEM((head_cols // 128, streams * 16, 128), F32),
            pltpu.VMEM((head_cols // 128, streams * 8, 128), F32),
            pltpu.VMEM(((frames + 1) * streams, head_cols), BF),
            pltpu.SemaphoreType.DMA((15,)),
        ],
        compiler_params=pltpu.CompilerParams(vmem_limit_bytes=WHOLE - 10 * 10**6),
        cost_estimate=pl.CostEstimate(flops=6 * 10**9, bytes_accessed=12 * 10**6, transcendentals=0),
        name="attend",
    )(fill, length, arrived, mate, memory, lkeys, lvalues, wq, wk, wv, wo, *pieces)


def feed_kernel(
    part_ref, mate_ref, inputs_ref, u0_ref, u1_ref, u2_ref, u3_ref, d0_ref, d1_ref, d2_ref, d3_ref,
    w_up_in, w_down_in, state_ref, next_ref, down_ref, w_up, w_down, sem,
):
    half = lax.axis_index("fsdp")
    other = pl.multiple_of((1 - half) * 512, 512)
    ups, downs = [], []
    for n, piece in enumerate((u0_ref, u1_ref, u2_ref, u3_ref)):
        row = pl.multiple_of(other + lax.rem(colour() + n, PARTS) * 128, 128)
        ups.append(pltpu.make_async_copy(piece, w_up.at[pl.ds(row, 128), :], sem.at[n]))
    for n, piece in enumerate((d0_ref, d1_ref, d2_ref, d3_ref)):
        row = pl.multiple_of(lax.rem(colour() + n, PARTS) * 512, 512)
        downs.append(
            pltpu.make_async_copy(piece, w_down.at[pl.ds(row, 512), pl.ds(other, 512)], sem.at[4 + n])
        )
    for copy in ups + downs:
        copy.start()
    frame_rows = inputs_ref.shape[0]
    attn_out = part_ref[...].astype(F32) + mate_ref[...].astype(F32)
    next_ref[...] = jnp.tanh(attn_out[frame_rows:, :]).astype(BF)
    state = inputs_ref[...].astype(F32) + attn_out[0:frame_rows, :]
    state_ref[...] = state
    h_norm = normalize(state).astype(BF)
    for copy in ups:
        copy.wait()
    hidden = jax.nn.gelu(matmul(h_norm, w_up[...]), approximate=True).astype(BF)
    for copy in downs:
        copy.wait()
    down_ref[...] = matmul(hidden, w_down[...]).astype(BF)


def feed(part, mate, inputs, up_pieces, down_pieces, staged):
    frame_rows, width = inputs.shape
    vmem = pl.BlockSpec(memory_space=pltpu.VMEM)
    hbm = pl.BlockSpec(memory_space=pltpu.HBM)
    w_up, w_down = staged
    return pl.pallas_call(
        feed_kernel,
        out_shape=(
            jax.ShapeDtypeStruct((frame_rows, width), F32),
            jax.ShapeDtypeStruct((part.shape[0] - frame_rows, width), BF),
            jax.ShapeDtypeStruct((frame_rows, width), BF),
            jax.ShapeDtypeStruct(w_up.shape, BF),
            jax.ShapeDtypeStruct(w_down.shape, BF),
        ),
        in_specs=[vmem] * 3 + [hbm] * 8 + [vmem] * 2,
        out_specs=(vmem,) * 5,
        input_output_aliases={11: 3, 12: 4},
        scratch_shapes=[pltpu.SemaphoreType.DMA((8,))],
        compiler_params=pltpu.CompilerParams(vmem_limit_bytes=ROOM),
        cost_estimate=pl.CostEstimate(flops=3 * 10**9, bytes_accessed=10 * 10**6, transcendentals=0),
        name="feed",
    )(part, mate, inputs, *up_pieces, *down_pieces, *staged)[0:3]


def finish_kernel(state_ref, down_ref, mate_ref, gain_ref, out_ref):
    down = down_ref[...].astype(F32) + mate_ref[...].astype(F32)
    result = normalize(state_ref[...] + down) * gain_ref[...]
    out_ref[...] = result.astype(BF).reshape(out_ref.shape)


def finish(state, down, mate, gain, streams):
    vmem = pl.BlockSpec(memory_space=pltpu.VMEM)
    return pl.pallas_call(
        finish_kernel,
        out_shape=jax.ShapeDtypeStruct((state.shape[0] // streams, streams, state.shape[1]), BF),
        in_specs=[vmem] * 4,
        out_specs=vmem,
        compiler_params=pltpu.CompilerParams(vmem_limit_bytes=ROOM),
        name="finish",
    )(state, down, mate, gain[None, :])


def shards(
    features, memory_bank, memory_fill, left_keys, left_values, left_length,
    w_query, w_key, w_value, w_out, w_up, w_down, out_gain,
):
    streams = memory_bank.shape[0]
    swap = [(0, 1), (1, 0)]
    ready, first, up, down = prepare(features, w_query, w_key, w_value, w_out, w_up, w_down)
    arrived = lax.all_to_all(ready, GRID, split_axis=0, concat_axis=0, tiled=True)
    first = hop(first, ACROSS)
    up = hop(up, ACROSS)
    down = hop(down, ACROSS)
    arrived_mate = lax.ppermute(arrived, "mp", swap)
    pieces = spread(first, TO_Z_BELOW)
    up_pieces = spread(up, TO_Z_ABOVE)
    down_pieces = spread(down, TO_Z_BELOW)
    staged_feed = stage_feed(w_up, w_down)
    inputs, part, center_keys, center_values = attend(
        memory_fill, left_length, arrived, arrived_mate, memory_bank, left_keys, left_values,
        w_query, w_key, w_value, w_out, pieces,
    )
    mate = lax.ppermute(part, "mp", swap)
    state, memory_next, down_part = feed(part, mate, inputs, up_pieces, down_pieces, staged_feed)
    down_mate = lax.ppermute(down_part, "mp", swap)
    out = finish(state, down_part, down_mate, out_gain, streams)
    return (jnp.transpose(out, (1, 0, 2)), memory_next, center_keys, center_values)


def solution(mesh):
    in_specs = (
        P(None, ("dp", "fsdp"), None),
        P(("dp", "fsdp"), None, None),
        P(("dp", "fsdp")),
        P(("dp", "fsdp"), None, "mp"),
        P(("dp", "fsdp"), None, "mp"),
        P(("dp", "fsdp")),
        P("fsdp", "mp"),
        P("fsdp", "mp"),
        P("fsdp", "mp"),
        P("mp", "fsdp"),
        P("fsdp", "mp"),
        P("mp", "fsdp"),
        P(),
    )
    out_specs = (
        P(("dp", "fsdp"), None, None),
        P(("dp", "fsdp"), None),
        P(("dp", "fsdp"), None, "mp"),
        P(("dp", "fsdp"), None, "mp"),
    )

    return jax.shard_map(shards, mesh=mesh, in_specs=in_specs, out_specs=out_specs, check_vma=False)
```
